32 devices in a mesh: grp: 2 (over y), seq: 4 (over z), head: 2 (over x), rep: 2 (over core).
Axes of the slice: x: 2, y: 2, z: 4, core: 2. Of those that a mesh axis runs over, the one named last changes fastest.
Arguments:
- x_proj: bfloat16 [4, 4, 4, 32, 8192], P(('grp', 'rep'), None, 'seq', None, 'head'), parts along dimension 0, may hold values from -6 to 6
- gate_proj: bfloat16 [4, 4, 4, 32, 8192], P(('grp', 'rep'), None, 'seq', None, 'head'), parts along dimension 0, may hold values from -6 to 6
- bc_proj: bfloat16 [4, 4, 4, 32, 256], P(('grp', 'rep'), None, 'seq'), parts along dimension 0, may hold values from -6 to 6
- dt_proj: bfloat16 [4, 4, 4, 32, 128], P(('grp', 'rep'), None, 'seq', None, 'head'), parts along dimension 0, may hold values from -5.5 to 7.5
- a_rate: float32 [128], P('head'), may hold values from 0.0001953125 to 0.05
- dt_bias: float32 [128], P('head'), may hold values from -1 to 1
- d_skip: float32 [128], P('head'), may hold values from 0.5 to 1.5
- conv_x_weight: float32 [4, 8192], P(None, 'head'), may hold values from -3 to 3
- conv_bc_weight: float32 [4, 256], replicated, may hold values from -3 to 3
- norm_gain: float32 [8192], P('head'), may hold values from 0.1 to 1.9
- out_weight: bfloat16 [8192, 2048], P(('seq', 'rep'), 'head'), may hold values from -0.0625 to 0.0625
- request_first_position: int32 [4], P(('grp', 'rep')), parts along dimension 0, may hold values from 0 to 255
- owner: int32 [4, 4], P(('grp', 'rep')), parts along dimension 0, may hold values from 0 to 3, each once within a row
Outputs:
- mixed: bfloat16 [4, 512, 2048], P(('grp', 'rep'), 'seq', 'head'), parts along dimension 0
- ssm_state: float32 [4, 4, 128, 2048], P(('grp', 'rep'), 'seq', 'head'), parts along dimension 0
- conv_x_state: bfloat16 [4, 4, 3, 2048], P(('grp', 'rep'), 'seq', None, 'head'), parts along dimension 0
- conv_bc_state: bfloat16 [4, 4, 3, 64], P(('grp', 'rep'), 'seq'), parts along dimension 0
The draws below stay inside these ranges and needn't reach their ends.
There are 2 independent parts, one for each index of `grp`. The reference program is written for one: setup_inputs(seed, part) draws one part's arguments, and reference() takes and returns one part's arrays. A program takes and returns all parts, laid end to end along the dimension named above; an argument that names none is the same for every part. Nothing has to cross between parts.
Inputs may be any that keep to these rules, and one draw needn't show every extreme that they name: Each row of owner names every index of seq once.
All inputs are finite; a program needn't handle non-finite values.
Results may differ from the reference program's by a relative error of at most 0.007.
Values may be sent and summed in bfloat16 or wider, within the bound.
No kernel may reach another device: no remote copies, remote signals or barrier semaphores. Data moves between devices by JAX's collectives and lax.ppermute only.
A program may use at most 128 MiB of HBM per device.

```python
import jax
import jax.numpy as jnp
from jax import lax

D = 2048
HEADS = 128
HEAD_DIM = 64
NSTATE = 128
KCONV = 4
SPAN = 128
TOK_DEV = 128
INNER = 8192
LENGTH = 512
SUB = 32
REQS = 2
N_SEQ = 4
N_HEAD = 2


def draw_dt_proj(key, part):
    axis_extents = (REQS, N_SEQ, N_SEQ, SUB, HEADS)
    starting_displacement = 0.5 * jnp.clip(jax.random.normal(key, axis_extents, jnp.float32), -3.0, 3.0)
    block_offset = jax.random.uniform(jax.random.fold_in(key, 11), (REQS, N_SEQ, 1, 1, HEADS), jnp.float32, -2.5, 1.5)
    spots = jax.random.randint(jax.random.fold_in(key, 7), (REQS, 3, HEADS), 0, LENGTH)
    agreeing_tally = jnp.arange(LENGTH, dtype=jnp.int32)[None, :, None, None] == spots[:, None, :, :]
    segment_extent = jnp.any(agreeing_tally, axis=2).astype(jnp.float32) * 4.0
    return (starting_displacement + block_offset + segment_extent.reshape(axis_extents)).astype(jnp.bfloat16)


def draw_a_rate(key, part):
    share = 0.5
    picked = jax.random.uniform(jax.random.fold_in(key, 1), (HEADS,), jnp.float32)
    level = jax.random.uniform(jax.random.fold_in(key, 2), (HEADS,), jnp.float32)
    slow_rate = jnp.exp(jnp.log(0.3 / LENGTH) + level * jnp.log(2.0 / 0.3))
    quick_decay_speed = jnp.exp(jnp.log(1.0 / LENGTH) + level * jnp.log(0.05 * LENGTH))
    return jnp.where(picked < share, slow_rate, quick_decay_speed).astype(jnp.float32)


def shard_levels(rng, shape, cuts, least, high):
    loudness, own = 1.0, jax.random.fold_in(rng, 6)
    for dim, shards_of in cuts:
        draws = jnp.exp(jax.random.uniform(jax.random.fold_in(own, dim), (shards_of,), jnp.float32, least / len(cuts), high / len(cuts)))
        loudness = loudness * jnp.repeat(draws, shape[dim] // shards_of).reshape([-1 if axis == dim else 1 for axis in range(len(shape))])
    return loudness


def normal_values(key, dims, width, most, pieces=(), kind=jnp.bfloat16):
    loudness = shard_levels(key, dims, pieces, -0.22, 0.18) if pieces else 1.0
    array = jax.random.normal(key, dims, jnp.float32) * width * loudness
    return jnp.minimum(jnp.maximum(array, -most), most).astype(kind)


def setup_inputs(seed: int = 0, part: int = 0) -> dict:
    streams_of = jax.random.split(jax.random.key(seed), 14)
    part_keys = jax.random.split(jax.random.fold_in(streams_of[13], part), 14)
    x_proj = normal_values(part_keys[0], (REQS, N_SEQ, N_SEQ, SUB, INNER), 1.0, 6.0, ((0, 2), (2, 4), (4, 2)))
    gate_proj = normal_values(part_keys[1], (REQS, N_SEQ, N_SEQ, SUB, INNER), 1.0, 6.0, ((0, 2), (2, 4), (4, 2)))
    bc_proj = normal_values(part_keys[2], (REQS, N_SEQ, N_SEQ, SUB, 2 * NSTATE), 1.0, 6.0, ((0, 2), (2, 4)))
    dt_proj = draw_dt_proj(jax.random.fold_in(jax.random.fold_in(streams_of[13], part), 71), part)
    a_rate = draw_a_rate(jax.random.fold_in(streams_of[13], 71), part)
    dt_bias = jnp.clip(jax.random.uniform(streams_of[5], (HEADS,), jnp.float32, -1.0, 1.0) * shard_levels(streams_of[5], (HEADS,), ((0, 2),), -0.4, 0.0), -1.0, 1.0)
    d_skip = jnp.clip(0.5 + 1.0 * jax.random.uniform(streams_of[6], (HEADS,), jnp.float32) ** shard_levels(streams_of[6], (HEADS,), ((0, 2),), -0.2, 0.2), 0.5, 1.5)
    conv_x_weight = normal_values(streams_of[7], (KCONV, INNER), KCONV ** -0.5, 3.0, ((1, 2),), jnp.float32)
    conv_bc_weight = normal_values(streams_of[8], (KCONV, 2 * NSTATE), KCONV ** -0.5, 3.0, (), jnp.float32)
    norm_gain = jnp.clip(1.0 + 0.18 * jax.random.normal(streams_of[9], (INNER,), jnp.float32), 0.1, 1.9)
    out_weight = normal_values(streams_of[10], (INNER, D), INNER ** -0.5, 0.0625, ((0, 8), (1, 2)))
    request_first_position = jax.random.randint(part_keys[11], (REQS,), 0, LENGTH // 2).astype(jnp.int32)
    owner = jax.vmap(lambda own: jax.random.permutation(own, N_SEQ))(jax.random.split(part_keys[12], REQS)).reshape((REQS, N_SEQ)).astype(jnp.int32)
    return dict(x_proj=x_proj, gate_proj=gate_proj, bc_proj=bc_proj, dt_proj=dt_proj, a_rate=a_rate, dt_bias=dt_bias, d_skip=d_skip, conv_x_weight=conv_x_weight, conv_bc_weight=conv_bc_weight, norm_gain=norm_gain, out_weight=out_weight, request_first_position=request_first_position, owner=owner)


highest = lax.Precision.HIGHEST
stability_constant = 1e-05

def span_terms(x_conv, b_rows, c_rows, step_size, log_decay):
    cum_decay = jnp.cumsum(log_decay, axis=1)
    scores = jnp.einsum('kqn,ktn->kqt', c_rows.astype(jnp.float32), b_rows.astype(jnp.float32), precision=highest)
    cum_heads = jnp.swapaxes(cum_decay, 1, 2)
    step_heads = jnp.swapaxes(step_size, 1, 2)
    block_len = cum_decay.shape[1]
    causal = jnp.arange(block_len)[:, None] >= jnp.arange(block_len)[None, :]
    decay_gap = cum_heads[:, :, :, None] - cum_heads[:, :, None, :]
    seg_decay = jnp.exp(jnp.where(causal, decay_gap, -jnp.inf))
    weights = (scores[:, None] * seg_decay * step_heads[:, :, None, :]).astype(jnp.bfloat16)
    y_intra = jnp.einsum('khqt,kthp->kqhp', weights.astype(jnp.float32), x_conv.astype(jnp.float32), precision=highest)
    remaining_length = jnp.exp(cum_decay[:, -1:, :] - cum_decay)
    scaled = ((remaining_length * step_size)[..., None] * x_conv.astype(jnp.float32)).astype(jnp.bfloat16)
    states = jnp.einsum('kthp,ktn->khpn', scaled.astype(jnp.float32), b_rows.astype(jnp.float32), precision=highest)
    return (cum_decay, y_intra, states, jnp.exp(cum_decay[:, -1, :]))

def conv_silu(values, weight):
    length = values.shape[0]
    padded = jnp.concatenate([jnp.zeros((weight.shape[0] - 1, values.shape[1]), values.dtype), values], axis=0)
    accum = jnp.zeros(values.shape, jnp.float32)
    for offset in range(weight.shape[0]):
        accum = accum + weight[offset] * padded[offset:offset + length].astype(jnp.float32)
    return jax.nn.silu(accum)

def one_request(x_in, z_in, bc_in, dt_in, start, a_rate, dt_bias, d_skip, conv_x_weight, conv_bc_weight, norm_gain, out_weight):
    length = x_in.shape[0]
    is_live = jnp.arange(length, dtype=jnp.int32) >= start
    x_live = jnp.where(is_live[:, None], x_in, jnp.zeros_like(x_in))
    bc_live = jnp.where(is_live[:, None], bc_in, jnp.zeros_like(bc_in))
    x_conv = conv_silu(x_live, conv_x_weight).astype(jnp.bfloat16)
    bc_conv = conv_silu(bc_live, conv_bc_weight).astype(jnp.bfloat16)
    step_size = jax.nn.softplus(dt_in.astype(jnp.float32) + dt_bias) * is_live.astype(jnp.float32)[:, None]
    log_decay = -a_rate * step_size
    blocks = length // SPAN
    x_blocks = x_conv.reshape(blocks, SPAN, HEADS, HEAD_DIM)
    b_blocks = bc_conv[:, :NSTATE].reshape(blocks, SPAN, NSTATE)
    c_blocks = bc_conv[:, NSTATE:].reshape(blocks, SPAN, NSTATE)
    step_blocks = step_size.reshape(blocks, SPAN, HEADS)
    decay_blocks = log_decay.reshape(blocks, SPAN, HEADS)

    def advance(state, inputs):
        input_block, b_block, c_block, step_block, decay_block = inputs
        cum_decay, y_intra, block_state, block_decay = span_terms(input_block[None], b_block[None], c_block[None], step_block[None], decay_block[None])
        from_state = jnp.exp(cum_decay[0])[:, :, None] * jnp.einsum('qn,hpn->qhp', c_block.astype(jnp.float32), state, precision=highest)
        y_out = y_intra[0] + from_state + d_skip[:, None] * input_block.astype(jnp.float32)
        return (block_decay[0][:, None, None] * state + block_state[0], y_out)
    start_state = jnp.zeros((HEADS, HEAD_DIM, NSTATE), jnp.float32)
    final_state, y_all = lax.scan(advance, start_state, (x_blocks, b_blocks, c_blocks, step_blocks, decay_blocks))
    y_flat = y_all.reshape(length, HEADS * HEAD_DIM)
    gated = y_flat * jax.nn.silu(z_in.astype(jnp.float32))
    mean_square = lax.optimization_barrier(jnp.mean(gated * gated, axis=1, keepdims=True))
    normed = (gated * lax.rsqrt(mean_square + stability_constant) * norm_gain).astype(jnp.bfloat16)
    mixed = jnp.dot(normed, out_weight, preferred_element_type=jnp.float32).astype(jnp.bfloat16)
    rim_rows = KCONV - 1
    return (mixed, final_state, x_live[length - rim_rows:], bc_live[length - rim_rows:])

def reference(x_proj, gate_proj, bc_proj, dt_proj, a_rate, dt_bias, d_skip, conv_x_weight, conv_bc_weight, norm_gain, out_weight, request_first_position, owner):
    length = TOK_DEV * N_SEQ
    rim_rows = KCONV - 1
    mixed_list = []
    state_list = []
    tail_x_list = []
    tail_bc_list = []
    for request in range(x_proj.shape[0]):
        mixed, final_state, tail_x, tail_bc = one_request(x_proj[request].reshape(length, -1), gate_proj[request].reshape(length, -1), bc_proj[request].reshape(length, -1), dt_proj[request].reshape(length, -1), request_first_position[request], a_rate, dt_bias, d_skip, conv_x_weight, conv_bc_weight, norm_gain, out_weight)
        inverse = jnp.argsort(owner[request]).astype(jnp.int32)
        slabs = final_state.reshape(HEADS, N_SEQ, -1)[:, inverse]
        state_list.append(jnp.transpose(slabs, (1, 0, 2)))
        x_slabs = tail_x.reshape(rim_rows, N_HEAD, N_SEQ, -1)[:, :, inverse]
        tail_x_list.append(jnp.transpose(x_slabs, (2, 0, 1, 3)).reshape(N_SEQ, rim_rows, -1))
        bc_slabs = tail_bc.reshape(rim_rows, N_SEQ, -1)[:, inverse]
        tail_bc_list.append(jnp.transpose(bc_slabs, (1, 0, 2)))
        mixed_list.append(mixed)
    return (jnp.stack(mixed_list), jnp.stack(state_list), jnp.stack(tail_x_list), jnp.stack(tail_bc_list))
```

```python
import functools

import jax
import jax.numpy as jnp
from jax import lax
from jax.experimental import pallas as pl
from jax.experimental.pallas import tpu as pltpu
from jax.sharding import PartitionSpec as P

HEAD_DIM = 64
NSTATE = 128
KCONV = 4
LANES = 128
PAD = 16
EPS = 1e-05
AXES = ("seq", "head", "rep")

f32, bf16 = jnp.float32, jnp.bfloat16
highest = lax.Precision.HIGHEST
VMEM_LIMIT = 60 * 1024 * 1024


def loop(count, body, carry):
    if count <= 4:
        for i in range(count):
            carry = body(i, carry)
        return carry
    return lax.fori_loop(0, count, body, carry)


def rows_at(start, size):
    if isinstance(start, int):
        return pl.ds(start, size)
    return pl.ds(pl.multiple_of(start, 8), size)


def silu(v):
    return v / (1.0 + jnp.exp(-v))


def place(place_ref, pieces, scratch, blocks, offset=PAD):
    me = place_ref[0]
    if len(pieces) == 1:
        total = pieces[0].shape[0]
        scratch[pl.ds(offset, total), :] = pieces[0][...].astype(scratch.dtype)
        return
    rows = pieces[0].shape[0] // blocks
    for k, piece in enumerate(pieces):
        at = me ^ k
        for block in range(blocks):
            start = offset + block * rows * len(pieces) + at * rows
            scratch[rows_at(start, rows), :] = piece[
                pl.ds(block * rows, rows), :
            ].astype(scratch.dtype)


def aux_kernel(n, blocks, heads, place_ref, *refs):
    pieces, refs = refs[:n], refs[n:]
    taps, rates, bt_out, c_out, score_out, rows_out, cum_out, step_out, tail_out, buf = refs
    total = cum_out.shape[0]
    span = total // blocks
    width = 2 * NSTATE
    buf[pl.ds(0, PAD), :] = jnp.zeros((PAD, buf.shape[1]), f32)
    place(place_ref, pieces, buf, blocks)
    first = buf[pl.ds(PAD, total), width + 64 : width + 65] * 256.0
    first = first + buf[pl.ds(PAD, total), width + 65 : width + 66]
    position = lax.broadcasted_iota(jnp.int32, (total, 1), 0).astype(f32)
    live = (position >= first).astype(f32)
    buf[pl.ds(PAD, total), :width] = jnp.where(live > 0.0, buf[pl.ds(PAD, total), :width], 0.0)
    lane = lax.broadcasted_iota(jnp.int32, (total, LANES), 1)
    raw = buf[pl.ds(PAD, total), width : width + LANES] + rates[1:2, :]
    step = jnp.maximum(raw, 0.0) + jnp.log1p(jnp.exp(-jnp.abs(raw)))
    step = jnp.where(lane < heads, step * live, 0.0)
    decay = -rates[0:1, :] * step
    step_out[...] = jnp.where(lane == LANES - 1, live, step)
    tail_out[...] = buf[pl.ds(PAD + total - 8, 8), :width].astype(bf16)
    cum_out[...] = decay
    q = lax.broadcasted_iota(jnp.int32, (span, span), 0)
    t = lax.broadcasted_iota(jnp.int32, (span, span), 1)
    lower = (q >= t).astype(f32)

    def one(block, carry):
        base = block * span
        here = rows_at(base, span)
        cum = jnp.dot(lower, cum_out[here, :], precision=highest, preferred_element_type=f32)
        cum_out[here, :] = cum
        lanes = pl.ds(base, span) if isinstance(base, int) else pl.ds(pl.multiple_of(base, LANES), span)
        cum_t, step_t = cum.T, step_out[here, :].T
        for pair in range(heads // 2):
            rows_out[pair, 0:2, lanes] = cum_t[2 * pair : 2 * pair + 2]
            rows_out[pair, 2:4, lanes] = step_t[2 * pair : 2 * pair + 2]
        acc = jnp.zeros((span, width), f32)
        window = buf[rows_at(base + PAD - 8, span + 8), :width]
        for k in range(KCONV):
            lo = 8 - KCONV + 1 + k
            acc = acc + taps[k : k + 1, :] * window[lo : lo + span]
        conv = silu(acc)
        b_rows, c_rows = conv[:, :NSTATE], conv[:, NSTATE:].astype(bf16)
        bt = b_rows.astype(bf16).astype(f32).T.astype(bf16)
        bt_out[:, lanes] = bt
        c_out[here, :] = c_rows
        score_out[here, :] = jnp.dot(c_rows, bt, preferred_element_type=f32) * lower
        return carry

    loop(blocks, one, 0)


def scan_kernel(n, blocks, place_ref, *refs):
    pieces, refs = refs[:n], refs[n:]
    params, bt, c_all, scores, row_tables, cum_all, step_all = refs[:7]
    y_out, state_out, tail_out, buf, cum_e, step_e = refs[7:]
    total = y_out.shape[0]
    span = total // blocks
    pair = pl.program_id(0)
    buf[pl.ds(0, PAD), :] = jnp.zeros((PAD, LANES), f32)
    place(place_ref, pieces, buf, blocks)
    live = step_all[:, LANES - 1 :]
    buf[pl.ds(PAD, total), :] = jnp.where(live > 0.0, buf[pl.ds(PAD, total), :], 0.0)
    tail_out[...] = buf[pl.ds(PAD + total - 8, 8), :].astype(bf16)
    row = lax.broadcasted_iota(jnp.int32, (LANES, LANES), 0)
    lane = lax.broadcasted_iota(jnp.int32, (LANES, LANES), 1)
    spread = (row == 2 * pair + lane // HEAD_DIM).astype(f32)
    cum_e[...] = jnp.dot(cum_all[...], spread, precision=highest, preferred_element_type=f32)
    step_e[...] = jnp.dot(step_all[...], spread, precision=highest, preferred_element_type=f32)
    left = lax.broadcasted_iota(jnp.int32, (span, LANES), 1) < HEAD_DIM

    def one(block, state):
        base = block * span
        here = rows_at(base, span)
        lanes = pl.ds(base, span) if isinstance(base, int) else pl.ds(pl.multiple_of(base, LANES), span)
        acc = jnp.zeros((span, LANES), f32)
        window = buf[rows_at(base + PAD - 8, span + 8), :]
        for k in range(KCONV):
            lo = 8 - KCONV + 1 + k
            acc = acc + params[k : k + 1, :] * window[lo : lo + span]
        x_conv = silu(acc).astype(bf16)
        x_wide = x_conv.astype(f32)
        cum = cum_e[here, :]
        last = cum[span - 1 : span, :]
        score = scores[here, :]
        parts = []
        for j in range(2):
            cum_row = row_tables[0, j : j + 1, lanes]
            step_row = row_tables[0, 2 + j : 3 + j, lanes]
            gap = jnp.minimum(cum[:, j * HEAD_DIM : j * HEAD_DIM + 1] - cum_row, 0.0)
            mix = (score * jnp.exp(gap) * step_row).astype(bf16)
            parts.append(jnp.dot(mix, x_conv, preferred_element_type=f32))
        y = jnp.where(left, parts[0], parts[1])
        c_rows = c_all[here, :]
        high = state.astype(bf16)
        low = (state - high.astype(f32)).astype(bf16)
        entering = jnp.dot(c_rows, high, preferred_element_type=f32)
        entering = entering + jnp.dot(c_rows, low, preferred_element_type=f32)
        y_out[here, :] = y + jnp.exp(cum) * entering + params[5:6, :] * x_wide
        scaled = (jnp.exp(last - cum) * step_e[here, :] * x_wide).astype(bf16)
        new = jnp.dot(bt[:, lanes], scaled, preferred_element_type=f32)
        return jnp.exp(last) * state + new

    state = loop(blocks, one, jnp.zeros((NSTATE, LANES), f32))
    state_out[...] = state.T


def project_kernel(n, blocks, seq, tiles, place_ref, *refs):
    y_ref, refs = refs[0], refs[1:]
    gates, refs = refs[:n], refs[n:]
    gain, w_own, w_other, send_out, keep_out, gate_buf, feat, sums = refs
    step = pl.program_id(0)
    total = y_ref.shape[0]
    per = total // seq

    @pl.when(step == 0)
    def _():
        place(place_ref, gates, gate_buf, blocks, 0)

        def one(part, carry):
            here = rows_at(part * per, per)
            gate = gate_buf[here, :].astype(f32)
            gated = y_ref[here, :] * silu(gate)
            square = jnp.sum(gated * gated, axis=1, keepdims=True)
            sums[part] = jnp.broadcast_to(square, (per, LANES)).T[:8, :]
            feat[here, :] = (gated * gain[4:5, :]).astype(bf16)
            return carry

        loop(seq, one, 0)

    def write(out, weight, first):
        for part in range(seq) if seq <= 4 else ():
            out[part, :per, :] = jnp.dot(
                feat[pl.ds(part * per, per), :], weight[...], preferred_element_type=f32
            ).astype(bf16)
            out[part, per:, :] = jnp.zeros((8, out.shape[2]), bf16)
        if seq > 4:
            @pl.loop(0, seq)
            def _(part):
                out[part, :per, :] = jnp.dot(
                    feat[rows_at(part * per, per), :], weight[...], preferred_element_type=f32
                ).astype(bf16)
                out[part, per:, :] = jnp.zeros((8, out.shape[2]), bf16)

        @pl.when(step == first)
        def _():
            out[:, per:, :LANES] = sums[...].astype(bf16)

    sending = step < tiles
    own_now = jnp.where(sending, place_ref[1] == 0, place_ref[1] == 1)
    for phase, (out, first) in enumerate(((send_out, 0), (keep_out, tiles))):
        for own, weight in ((True, w_own), (False, w_other)):
            @pl.when((sending == (phase == 0)) & (own_now == own))
            def _(out=out, weight=weight, first=first):
                write(out, weight, first)


def finish_kernel(n, inner, *refs):
    parts, out = refs[:n], refs[n]
    per = out.shape[0]
    row = jnp.zeros((1, LANES), f32)
    for part in parts:
        row = row + part[per : per + 1, :LANES].astype(f32)
    scale = lax.rsqrt(row / inner + EPS)
    scale = jnp.broadcast_to(scale, (LANES, LANES)).T
    for at in range(0, out.shape[1], LANES):
        acc = jnp.zeros((per, LANES), f32)
        for part in parts:
            acc = acc + part[:per, at : at + LANES].astype(f32)
        out[:, at : at + LANES] = (acc * scale).astype(bf16)


def local(
    mesh_sizes,
    x_proj,
    gate_proj,
    bc_proj,
    dt_proj,
    a_rate,
    dt_bias,
    d_skip,
    conv_x_weight,
    conv_bc_weight,
    norm_gain,
    out_weight,
    request_first_position,
    owner,
):
    n, n_head, n_rep = mesh_sizes
    blocks, rows = x_proj.shape[1], x_proj.shape[3]
    per = blocks * rows
    total = per * n
    half_width = x_proj.shape[4]
    chans = half_width // n
    heads = chans // HEAD_DIM
    all_heads = dt_proj.shape[4]
    inner = half_width * n_head
    cols = out_weight.shape[1]
    group = n // n_head
    fast = rows % 16 == 0

    def dev(s, h, c):
        return (s * n_head + h) * n_rep + c

    def pairs(rule):
        return [
            (dev(s, h, c), dev(*rule(s, h, c)))
            for s in range(n)
            for h in range(n_head)
            for c in range(n_rep)
        ]

    def move(value, rule):
        return lax.ppermute(value, AXES, pairs(rule))

    def swap(s, h, c):
        return (s, c, h)

    seq_at, head_at, rep_at = (lax.axis_index(axis) for axis in AXES)
    me = (seq_at % group) * n_rep + rep_at
    half = seq_at // group

    x_in = x_proj.reshape(per, half_width)
    gate_in = gate_proj.reshape(per, half_width)
    bc_in = bc_proj.reshape(per, -1)
    dt_in = dt_proj.reshape(per, all_heads)
    x_turned = move(x_in, swap)

    start = request_first_position[0]
    digits = jnp.stack([start // 256, start % 256])
    facts = jnp.concatenate([digits, owner[0]]).astype(bf16)
    facts = jnp.broadcast_to(facts[None], (per, n + 2))
    aux_pad = jnp.zeros((per, 64 - heads), bf16)
    aux_end = jnp.zeros((per, 64 - n - 2), bf16)

    def aux_for(m):
        mine = lax.dynamic_slice(dt_in, (0, m * heads), (per, heads))
        return jnp.concatenate([bc_in, mine, aux_pad, facts, aux_end], axis=1)

    aux = [
        move(
            aux_for(seq_at ^ k),
            lambda s, h, c: (h * group + (s ^ k) // n_rep, c, (s ^ k) % n_rep),
        )
        for k in range(n)
    ]
    gate_turned = move(gate_in, swap)

    own_chan = me * chans
    taps = lax.dynamic_slice(conv_x_weight, (0, own_chan), (KCONV, chans))
    gain = lax.dynamic_slice(norm_gain, (own_chan,), (chans,))[None]

    def per_head(vector):
        return lax.dynamic_slice(vector, (me * heads,), (heads,))

    vectors = [per_head(v) for v in (d_skip, a_rate, dt_bias)]
    skip_wide = jnp.repeat(vectors[0], HEAD_DIM)[None]
    flat = jnp.concatenate(
        [vectors[1], jnp.zeros((64 - heads,), f32), vectors[2], jnp.zeros((64 - heads,), f32)]
    )
    flat = jnp.concatenate([flat, jnp.zeros((chans - 2 * 64,), f32)])[None]
    packed = jnp.concatenate([taps, gain, skip_wide, flat, jnp.zeros((1, chans), f32)], axis=0)
    other = lax.ppermute(packed, "head", [(i, (i + 1) % n_head) for i in range(n_head)])
    params = jnp.where(head_at == half, packed, other)
    rates = jnp.zeros((8, LANES), f32)
    rates = rates.at[0, :heads].set(params[6, :heads]).at[1, :heads].set(params[6, 64 : 64 + heads])

    place_info = jnp.stack([me, (head_at == rep_at).astype(jnp.int32)]).astype(jnp.int32)

    def spread(value, width):
        def rule(k):
            return lambda s, h, c: (c * group + (s ^ k) // n_rep, h, (s ^ k) % n_rep)

        return [
            move(lax.dynamic_slice(value, (0, (seq_at ^ k) * width), (per, width)), rule(k))
            for k in range(n)
        ]

    def gathered(pieces):
        if fast:
            return pieces
        width = pieces[0].shape[1]
        full = jnp.zeros((blocks, n, rows, width), pieces[0].dtype)
        for k, piece in enumerate(pieces):
            full = lax.dynamic_update_slice(
                full, piece.reshape(blocks, 1, rows, width), (0, me ^ k, 0, 0)
            )
        return [full.reshape(total, width)]

    x_pieces = spread(x_turned, chans)
    w_other_in, gate_turned = lax.optimization_barrier((out_weight, gate_turned))
    w_other = lax.ppermute(w_other_in, "head", [(i, (i + 1) % n_head) for i in range(n_head)])
    gate_pieces = spread(gate_turned, chans)

    def whole(shape):
        return pl.BlockSpec(shape, lambda *_: (0,) * len(shape))

    def call(kernel, grid, in_specs, out_specs, out_shape, scratch, cost, name):
        return pl.pallas_call(
            kernel,
            grid_spec=pltpu.PrefetchScalarGridSpec(
                num_scalar_prefetch=1,
                grid=grid,
                in_specs=in_specs,
                out_specs=out_specs,
                scratch_shapes=scratch,
            ),
            out_shape=out_shape,
            compiler_params=pltpu.CompilerParams(vmem_limit_bytes=VMEM_LIMIT),
            cost_estimate=pl.CostEstimate(flops=cost, bytes_accessed=4 << 20, transcendentals=0),
            name=name,
        )

    shape = jax.ShapeDtypeStruct
    aux_pieces = gathered(aux)
    aux_shapes = [
        ((NSTATE, total), bf16),
        ((total, NSTATE), bf16),
        ((total, LANES), f32),
        ((heads // 2, 8, total), f32),
        ((total, LANES), f32),
        ((total, LANES), f32),
        ((8, 2 * NSTATE), bf16),
    ]
    tables = call(
        functools.partial(aux_kernel, len(aux_pieces), blocks, heads),
        (1,),
        [whole(piece.shape) for piece in aux_pieces]
        + [whole(conv_bc_weight.shape), whole((8, LANES))],
        [whole(s) for s, _ in aux_shapes],
        [shape(s, d) for s, d in aux_shapes],
        [pltpu.VMEM((total + PAD, aux_pieces[0].shape[1]), f32)],
        3_000_000_000,
        "aux",
    )(place_info, *aux_pieces, conv_bc_weight, rates)
    table_ins, tail_bc = list(tables[:6]), tables[6]

    x_ready = gathered(x_pieces)
    y, state, tail_x = call(
        functools.partial(scan_kernel, len(x_ready), blocks),
        (chans // LANES,),
        [pl.BlockSpec((piece.shape[0], LANES), lambda i, _: (0, i)) for piece in x_ready]
        + [pl.BlockSpec((8, LANES), lambda i, _: (0, i))]
        + [whole(s) for s, _ in aux_shapes[:3]]
        + [pl.BlockSpec((1, 8, total), lambda i, _: (i, 0, 0))]
        + [whole(s) for s, _ in aux_shapes[4:6]],
        [
            pl.BlockSpec((total, LANES), lambda i, _: (0, i)),
            pl.BlockSpec((LANES, NSTATE), lambda i, _: (i, 0)),
            pl.BlockSpec((8, LANES), lambda i, _: (0, i)),
        ],
        [shape((total, chans), f32), shape((chans, NSTATE), f32), shape((8, chans), bf16)],
        [
            pltpu.VMEM((total + PAD, LANES), f32),
            pltpu.VMEM((total, LANES), f32),
            pltpu.VMEM((total, LANES), f32),
        ],
        8_000_000_000,
        "scan",
    )(place_info, *x_ready, params, *table_ins)

    owner_here = aux[0][0, 2 * NSTATE + 66 : 2 * NSTATE + 66 + n].astype(jnp.int32)
    slabs = state.astype(bf16).reshape(heads, n, HEAD_DIM // n, NSTATE)
    rim = KCONV - 1
    tail_rows = tail_x[8 - rim :].reshape(rim * chans // LANES, LANES)
    bc_slabs = tail_bc[8 - rim :].reshape(rim, n, -1)
    bc_wide = bc_slabs.shape[2]
    slab_rows = heads * (HEAD_DIM // n)
    tail_count = rim * chans // LANES

    def state_for(target):
        slab = jnp.sum(jnp.where(owner_here == target, jnp.arange(n, dtype=jnp.int32), 0))
        mine = lax.dynamic_slice(slabs, (0, slab, 0, 0), (heads, 1, HEAD_DIM // n, NSTATE))
        mine = mine.reshape(slab_rows, NSTATE)
        rims = jnp.where(slab == me, tail_rows, jnp.zeros_like(tail_rows))
        bc_one = lax.dynamic_slice(bc_slabs, (0, slab, 0), (rim, 1, bc_wide)).reshape(rim, bc_wide)
        bc_one = jnp.pad(bc_one, ((0, 8 - rim), (0, LANES - bc_wide)))
        return jnp.concatenate([mine, rims, bc_one], axis=0)

    def state_rule(k):
        return lambda s, h, c: (((s % group) * n_rep + c) ^ k, s // group, h)

    state_parts = [move(state_for(me ^ k), state_rule(k)) for k in range(n)]
    ssm = jnp.zeros((all_heads, HEAD_DIM // n, NSTATE), f32)
    rim_x = jnp.zeros((tail_count, LANES), bf16)
    for k, part in enumerate(state_parts):
        block = part[:slab_rows].astype(f32).reshape(heads, HEAD_DIM // n, NSTATE)
        ssm = lax.dynamic_update_slice(ssm, block, ((seq_at ^ k) * heads, 0, 0))
        rim_x = rim_x + part[slab_rows : slab_rows + tail_count]
    ssm_state = ssm.reshape(1, 1, all_heads, HEAD_DIM // n * NSTATE)
    conv_x_state = rim_x.reshape(1, 1, rim, chans)
    bc_rows = state_parts[0][slab_rows + tail_count :]
    conv_bc_state = bc_rows[:rim, :bc_wide][None, None]

    gate_ready = gathered(gate_pieces)
    tile = min(256, cols)
    tiles = cols // tile

    def weight_at(phase_of_own):
        def index(j, info):
            mine = jnp.where(info[1] == 0, 0, 1) if phase_of_own else jnp.where(info[1] == 0, 1, 0)
            return (0, jnp.clip(j - mine * tiles, 0, tiles - 1))

        return index

    send, keep = call(
        functools.partial(project_kernel, len(gate_ready), blocks, n, tiles),
        (2 * tiles,),
        [whole((total, chans))]
        + [whole(piece.shape) for piece in gate_ready]
        + [
            whole((8, chans)),
            pl.BlockSpec((chans, tile), weight_at(True)),
            pl.BlockSpec((chans, tile), weight_at(False)),
        ],
        [
            pl.BlockSpec((n, per + 8, tile), lambda j, _: (0, 0, jnp.minimum(j, tiles - 1))),
            pl.BlockSpec((n, per + 8, tile), lambda j, _: (0, 0, jnp.maximum(j - tiles, 0))),
        ],
        [shape((n, per + 8, cols), bf16)] * 2,
        [
            pltpu.VMEM((total, chans), bf16),
            pltpu.VMEM((total, chans), bf16),
            pltpu.VMEM((n, 8, LANES), f32),
        ],
        4_000_000_000,
        "project",
    )(place_info, y, *gate_ready, params, out_weight, w_other)

    came = lax.ppermute(send, "rep", [(i, (i + 1) % n_rep) for i in range(n_rep)])

    def sum_for(target):
        def pick(value):
            return lax.dynamic_index_in_dim(value, target, 0, keepdims=False).astype(f32)

        return (pick(keep) + pick(came)).astype(bf16)

    def final_rule(k):
        return lambda s, h, c: (s ^ k, c, h)

    parts = [move(sum_for(seq_at ^ k), final_rule(k)) for k in range(n)]
    mixed = pl.pallas_call(
        functools.partial(finish_kernel, n, float(inner)),
        out_shape=shape((per, cols), bf16),
        compiler_params=pltpu.CompilerParams(vmem_limit_bytes=VMEM_LIMIT),
        name="finish",
    )(*parts)
    return (mixed[None], ssm_state, conv_x_state, conv_bc_state)


SPAN = 128
INNER = 8192
stability_constant = EPS


def passed_along(value, axis, by):
    devices = lax.axis_size(axis)
    pairs = [(i, i + by) for i in range(devices) if 0 <= i + by < devices]
    return lax.ppermute(value, axis, pairs)


def prefix(value, axis, combine, identity, reverse):
    devices, place = (lax.axis_size(axis), lax.axis_index(axis))
    everything = jax.tree.map(lambda part: lax.all_gather(part, axis), value)
    start = jax.tree.map(
        lambda part, zero: jnp.broadcast_to(jnp.asarray(zero, part.dtype), part.shape),
        value,
        identity,
    )

    def lap(k, before):
        at = devices - 1 - k if reverse else k
        reached = at > place if reverse else at < place
        new = combine(before, jax.tree.map(lambda part: part[at], everything))
        return jax.tree.map(lambda a, b: jnp.where(reached, a, b), new, before)

    return lax.fori_loop(0, devices, lap, start)


def broadcast(block, axis, source):
    block = jnp.where(lax.axis_index(axis) == source, block, jnp.zeros_like(block))
    return lax.psum(block, axis)


def span_terms(x_conv, b_rows, c_rows, step_size, log_decay):
    cum_decay = jnp.cumsum(log_decay, axis=1)
    scores = jnp.einsum("kqn,ktn->kqt", c_rows, b_rows, preferred_element_type=jnp.float32)
    cum_heads = jnp.swapaxes(cum_decay, 1, 2)
    step_heads = jnp.swapaxes(step_size, 1, 2)
    block_len = cum_decay.shape[1]
    causal = jnp.arange(block_len)[:, None] >= jnp.arange(block_len)[None, :]
    decay_gap = cum_heads[:, :, :, None] - cum_heads[:, :, None, :]
    seg_decay = jnp.exp(jnp.where(causal, decay_gap, -jnp.inf))
    weights = (scores[:, None] * seg_decay * step_heads[:, :, None, :]).astype(jnp.bfloat16)
    y_intra = jnp.einsum("khqt,kthp->kqhp", weights, x_conv, preferred_element_type=jnp.float32)
    remaining_length = jnp.exp(cum_decay[:, -1:, :] - cum_decay)
    scaled = ((remaining_length * step_size)[..., None] * x_conv.astype(jnp.float32)).astype(
        jnp.bfloat16
    )
    states = jnp.einsum("kthp,ktn->khpn", scaled, b_rows, preferred_element_type=jnp.float32)
    return (cum_decay, y_intra, states, jnp.exp(cum_decay[:, -1, :]))


def conv_silu(preceding_tokens, current, weight):
    extended = jnp.concatenate([preceding_tokens, current], axis=0)
    length = current.shape[0]
    accum = jnp.zeros(current.shape, jnp.float32)
    for offset in range(weight.shape[0]):
        accum = accum + weight[offset] * extended[offset : offset + length].astype(jnp.float32)
    return jax.nn.silu(accum)


def link(preceding_tokens, later):
    return (
        preceding_tokens[0] * later[0],
        later[0][:, None, None] * preceding_tokens[1] + later[1],
    )


def multiply(preceding_tokens, later):
    return preceding_tokens * later


def add_rows(source, piece):
    return jnp.dot(source, piece, preferred_element_type=jnp.float32)


def take_slab(values, slab_index, seq_count):
    grouped = values.reshape(values.shape[0], seq_count, -1)
    return lax.dynamic_index_in_dim(grouped, slab_index, axis=1, keepdims=False)


def general(
    x_proj,
    gate_proj,
    bc_proj,
    dt_proj,
    a_rate,
    dt_bias,
    d_skip,
    conv_x_weight,
    conv_bc_weight,
    norm_gain,
    out_weight,
    request_first_position,
    owner,
):
    x_all, z_all, bc_all, dt_all = (
        lax.all_to_all(x_proj, "seq", split_axis=1, concat_axis=2, tiled=True),
        lax.all_to_all(gate_proj, "seq", split_axis=1, concat_axis=2, tiled=True),
        lax.all_to_all(bc_proj, "seq", split_axis=1, concat_axis=2, tiled=True),
        lax.all_to_all(dt_proj, "seq", split_axis=1, concat_axis=2, tiled=True),
    )
    tokens_here = x_all.shape[2] * x_all.shape[3]
    x_local = x_all.reshape(tokens_here, x_all.shape[4])
    z_local = z_all.reshape(tokens_here, z_all.shape[4])
    bc_local = bc_all.reshape(tokens_here, bc_all.shape[4])
    dt_local = dt_all.reshape(tokens_here, dt_all.shape[4])
    heads = dt_local.shape[1]
    seq_index = lax.axis_index("seq")
    seq_count = lax.axis_size("seq")
    positions = seq_index * tokens_here + jnp.arange(tokens_here, dtype=jnp.int32)
    is_live = positions >= request_first_position[0]
    x_live = jnp.where(is_live[:, None], x_local, jnp.zeros_like(x_local))
    bc_live = jnp.where(is_live[:, None], bc_local, jnp.zeros_like(bc_local))
    rim_rows = KCONV - 1
    tail_x = x_live[tokens_here - rim_rows :]
    tail_bc = bc_live[tokens_here - rim_rows :]
    before_x, before_bc = passed_along((tail_x, tail_bc), "seq", 1)
    x_conv = conv_silu(before_x, x_live, conv_x_weight).astype(jnp.bfloat16)
    bc_conv = conv_silu(before_bc, bc_live, conv_bc_weight).astype(jnp.bfloat16)
    step_size = (
        jax.nn.softplus(dt_local.astype(jnp.float32) + dt_bias)
        * is_live.astype(jnp.float32)[:, None]
    )
    log_decay = -a_rate * step_size
    blocks = tokens_here // SPAN
    x_blocks = x_conv.reshape(blocks, SPAN, heads, HEAD_DIM)
    b_blocks = bc_conv[:, :NSTATE].reshape(blocks, SPAN, NSTATE)
    c_blocks = bc_conv[:, NSTATE:].reshape(blocks, SPAN, NSTATE)
    cum_decay, y_intra, states, decays = span_terms(
        x_blocks,
        b_blocks,
        c_blocks,
        step_size.reshape(blocks, SPAN, heads),
        log_decay.reshape(blocks, SPAN, heads),
    )

    def advance(carry, inputs):
        factor, contrib = inputs
        return (factor[:, None, None] * carry + contrib, carry)

    zero_state = jnp.zeros((heads, HEAD_DIM, NSTATE), jnp.float32)
    local_final, local_enter = lax.scan(advance, zero_state, (decays, states))
    dev_decay = jnp.prod(decays, axis=0)
    ones_heads = jnp.ones((heads,), jnp.float32)
    enter_decay, enter_state = prefix(
        (dev_decay, local_final), "seq", link, (ones_heads, zero_state), False
    )
    c_wide = c_blocks.astype(jnp.float32)
    before_block = jnp.concatenate([ones_heads[None], jnp.cumprod(decays, axis=0)[:-1]], axis=0)
    entering = local_enter + before_block[:, :, None, None] * enter_state[None]
    y_state = jnp.exp(cum_decay)[..., None] * jnp.einsum(
        "kqn,khpn->kqhp", c_wide, entering, precision=highest
    )
    y_total = y_intra + y_state + d_skip[:, None] * x_blocks.astype(jnp.float32)
    y_flat = y_total.reshape(tokens_here, heads * HEAD_DIM)
    gated = y_flat * jax.nn.silu(z_local.astype(jnp.float32))
    square_sums = lax.psum(jnp.sum(gated * gated, axis=1), "head")
    normed = (
        gated * lax.rsqrt(square_sums[:, None] / INNER + stability_constant) * norm_gain
    ).astype(jnp.bfloat16)
    last_index = seq_count - 1
    after_decay = prefix(dev_decay, "seq", multiply, ones_heads, True)
    final_state = lax.psum(after_decay[:, None, None] * local_final, "seq")
    keep_x, keep_bc = (broadcast(tail_x, "seq", last_index), broadcast(tail_bc, "seq", last_index))
    slab_index = jnp.sum(
        jnp.where(owner[0] == seq_index, jnp.arange(seq_count, dtype=jnp.int32), 0)
    )
    ssm_state = take_slab(final_state.reshape(heads, -1), slab_index, seq_count)[None, None]
    conv_x_state = take_slab(keep_x, slab_index, seq_count)[None, None]
    conv_bc_state = take_slab(keep_bc, slab_index, seq_count)[None, None]
    features = lax.all_gather(normed, "head", axis=1, tiled=True)
    out_cols = out_weight.shape[1]
    mixed_sum = add_rows(features, lax.all_gather(out_weight, ("seq", "rep"), axis=0, tiled=True))
    mixed = mixed_sum.astype(jnp.bfloat16).reshape(1, tokens_here, out_cols)
    return (mixed, ssm_state, conv_x_state, conv_bc_state)


def solution(mesh):
    sizes = tuple(mesh.shape[axis] for axis in AXES)
    n, n_head, n_rep = sizes
    turned = n_head == n_rep == 2 and n & (n - 1) == 0
    return jax.shard_map(
        functools.partial(local, sizes) if turned else general,
        mesh=mesh,
        in_specs=(
            P(("grp", "rep"), None, "seq", None, "head"),
            P(("grp", "rep"), None, "seq", None, "head"),
            P(("grp", "rep"), None, "seq", None, None),
            P(("grp", "rep"), None, "seq", None, "head"),
            P("head"),
            P("head"),
            P("head"),
            P(None, "head"),
            P(),
            P("head"),
            P(("seq", "rep"), "head"),
            P(("grp", "rep")),
            P(("grp", "rep"), None),
        ),
        out_specs=(
            P(("grp", "rep"), "seq", "head"),
            P(("grp", "rep"), "seq", "head", None),
            P(("grp", "rep"), "seq", None, "head"),
            P(("grp", "rep"), "seq", None, None),
        ),
        check_vma=False,
    )
```
